32 devices in a mesh: seq: 8 (over z, x), head: 4 (over y, core).
Axes of the slice: x: 2, y: 2, z: 4, core: 2. Of those that a mesh axis runs over, the one named last changes fastest.
Arguments:
- video_q: bfloat16 [1024, 4096], P(('seq', 'head')), may hold values from -200 to 200
- video_k: bfloat16 [1024, 4096], P(('seq', 'head')), may hold values from -6 to 6
- video_v: bfloat16 [1024, 4096], P(('seq', 'head')), may hold values from -6 to 6
- text_k: bfloat16 [512, 4096], P(None, 'head'), may hold values from -6 to 6
- text_v: bfloat16 [512, 4096], P(None, 'head'), may hold values from -6 to 6
- out_weight: bfloat16 [4096, 5120], P('head'), may hold values from -0.09375 to 0.09375
Outputs:
- video_out: bfloat16 [1024, 5120], P(('seq', 'head'))
The draws below stay inside these ranges and needn't reach their ends.
All inputs are finite; a program needn't handle non-finite values.
Results may differ from the reference program's by a relative error of at most 0.018.
Values may be sent and summed in bfloat16 or wider, within the bound.
A program may use at most 128 MiB of HBM per device.

```python
import jax
import jax.numpy as jnp
from jax import lax

D = 5120
HEADS = 32
HD = 128
TEXT = 512
TOKENS = 1024
N_HEAD = 4


def paired_draw(key):
    shape = (TOKENS, HEADS * HD)
    key_rows = jnp.clip(jax.random.normal(jax.random.fold_in(key, 11), shape, jnp.float32), -6.0, 6.0)
    queries = jnp.clip(jax.random.normal(jax.random.fold_in(key, 12), shape, jnp.float32), -6.0, 6.0)
    return (queries, key_rows)


def draw_video_q(key, part):
    queries, key_rows = paired_draw(key)
    return queries.astype(jnp.bfloat16)


def draw_video_k(key, part):
    queries, key_rows = paired_draw(key)
    return key_rows.astype(jnp.bfloat16)


def block_levels(rng, extent, pieces, low, largest):
    def one(position, blocks):
        draws = jax.random.uniform(jax.random.fold_in(jax.random.fold_in(rng, 6), position), (blocks,), jnp.float32, low / len(pieces), largest / len(pieces))
        return jnp.repeat(jnp.exp(draws), extent[position] // blocks).reshape((-1,) + (1,) * (len(extent) - position - 1))

    loudness = one(*pieces[0])
    for cut in pieces[1:]:
        loudness = loudness * one(*cut)
    return loudness


def normal_values(own_key, shape, scale, most, split=(), dtype=jnp.bfloat16):
    values = jax.random.normal(own_key, shape, jnp.float32) * scale
    if len(split) > 0:
        values = block_levels(own_key, shape, split, -0.22, 0.18) * values
    return jnp.clip(values, min=-most, max=most).astype(dtype)


def setup_inputs(seed: int = 0) -> dict:
    arg_keys = jax.random.split(jax.random.key(seed), 7)
    video_q = draw_video_q(jax.random.fold_in(arg_keys[6], 71), 0)
    video_k = draw_video_k(jax.random.fold_in(arg_keys[6], 71), 0)
    video_v = normal_values(arg_keys[2], (TOKENS, HEADS * HD), 1.0, 6.0, ((0, 32),))
    text_k = normal_values(arg_keys[3], (TEXT, HEADS * HD), 1.0, 6.0, ((1, 4),))
    text_v = normal_values(arg_keys[4], (TEXT, HEADS * HD), 1.0, 6.0, ((1, 4),))
    out_weight = normal_values(arg_keys[5], (HEADS * HD, D), (HEADS * HD) ** -0.5, 0.09375, ((0, 4),))
    return {"video_q": video_q, "video_k": video_k, "video_v": video_v, "text_k": text_k, "text_v": text_v, "out_weight": out_weight}


def head_output(operands):
    queries, key_rows, value_rows = operands
    scores = jnp.dot(queries, key_rows.T, preferred_element_type=jnp.float32) * (HD ** -0.5)
    row_max = jnp.max(scores, axis=1, keepdims=True)
    weights = jnp.exp(scores - row_max).astype(jnp.bfloat16)
    totals = jnp.sum(weights.astype(jnp.float32), axis=1, keepdims=True)
    summed = jnp.dot(weights, value_rows, preferred_element_type=jnp.float32)
    return (summed / totals).astype(jnp.bfloat16)


def split_heads(array):
    return array.reshape(array.shape[0], HEADS, HD).transpose(1, 0, 2)


def reference(video_q, video_k, video_v, text_k, text_v, out_weight):
    tokens = video_q.shape[0]
    all_keys = jnp.concatenate([split_heads(video_k), split_heads(text_k)], axis=1)
    all_values = jnp.concatenate([split_heads(video_v), split_heads(text_v)], axis=1)
    attended = lax.map(head_output, (split_heads(video_q), all_keys, all_values))
    attended = attended.transpose(1, 0, 2).reshape(tokens, HEADS * HD)
    group_width = HEADS * HD // N_HEAD
    group_inputs = attended.reshape(tokens, N_HEAD, group_width).transpose(1, 0, 2)
    weight_groups = out_weight.reshape(N_HEAD, group_width, D)

    def add_group(summed_out, operands):
        part_in, part_weight = operands
        partial_out = jnp.dot(part_in, part_weight, preferred_element_type=jnp.float32).astype(jnp.bfloat16)
        partial_out = lax.optimization_barrier(partial_out)
        return summed_out + partial_out.astype(jnp.float32), None

    summed_out, unused = lax.scan(add_group, jnp.zeros((tokens, D), jnp.float32), (group_inputs, weight_groups))
    return summed_out.astype(jnp.bfloat16)
```

```python
import functools
import math

import jax
import jax.numpy as jnp
from jax import lax
from jax.experimental import pallas as pl
from jax.experimental.pallas import tpu as pltpu
from jax.sharding import PartitionSpec as P

HD = 128
BF16 = jnp.bfloat16
F32 = jnp.float32
CORES = 2
SCALE = HD ** (-0.5) * math.log2(math.e)


def kernel(
    n_seq, n_head, q_ref, k_ref, v_ref, tk_ref, tv_ref, w_ref, o_ref,
    stage, kq, vals, tk, tv, w, probs, att_send, att, part, pair_in, y_send, y_in,
    load_sem, text_sem, w_sem, kq_send, kq_recv, v_send, v_recv,
    att_ssem, att_rsem, pair_ssem, pair_rsem, y_ssem, y_rsem,
):
    s, g = lax.axis_index("seq"), lax.axis_index("head")
    core, chip = lax.rem(g, CORES), lax.div(g, CORES)
    chips = n_head // CORES
    rows = q_ref.shape[0]
    n_cols = w_sem.shape[0]
    width = w_ref.shape[1] // n_cols
    per_chunk = probs.shape[1] // (CORES * rows)
    chunks = n_seq // per_chunk

    def lanes(block):
        return pl.ds(pl.multiple_of(block * HD, HD), HD)

    def cols(n):
        return pl.ds(n * width, width)

    loads = [
        pltpu.make_async_copy(ref, stage.at[i], load_sem.at[i])
        for i, ref in enumerate((k_ref, q_ref, v_ref))
    ]
    texts = [
        pltpu.make_async_copy(tk_ref.at[:, lanes(s)], tk, text_sem.at[0]),
        pltpu.make_async_copy(tv_ref.at[:, lanes(s)], tv, text_sem.at[1]),
    ]
    weights = [
        pltpu.make_async_copy(w_ref.at[:, cols(n)], w.at[:, cols(n)], w_sem.at[n])
        for n in range(n_cols)
    ]
    for copy in loads + texts + weights:
        copy.start()

    others = [
        (lax.rem(s + d // n_head, n_seq), lax.rem(g + d % n_head, n_head))
        for d in range(1, n_seq * n_head)
    ]
    barrier = pltpu.get_barrier_semaphore()
    for ts, tg in others:
        pl.semaphore_signal(
            barrier, inc=1, device_id={"seq": ts, "head": tg},
            device_id_type=pl.DeviceIdType.MESH,
        )
    pl.semaphore_wait(barrier, len(others))

    def send(src, dst, ssem, rsem, ts, tg):
        copy = pltpu.make_async_remote_copy(
            src_ref=src, dst_ref=dst, send_sem=ssem, recv_sem=rsem,
            device_id={"seq": ts, "head": tg}, device_id_type=pl.DeviceIdType.MESH,
        )
        copy.start()
        return copy

    def wait_for(ref, sem):
        pltpu.make_async_copy(ref, ref, sem).wait()

    loads[0].wait()
    loads[1].wait()
    for ts, tg in others:
        send(stage.at[0:2, :, lanes(tg * n_seq + ts)], kq.at[:, s, g], kq_send, kq_recv, ts, tg)
    mine = lanes(g * n_seq + s)
    pltpu.make_async_copy(stage.at[0:2, :, mine], kq.at[:, s, g], kq_recv).start()
    loads[2].wait()
    for ts, tg in others:
        send(stage.at[2, :, lanes(tg * n_seq + ts)], vals.at[s, g], v_send, v_recv, ts, tg)
    pltpu.make_async_copy(stage.at[2, :, mine], vals.at[s, g], v_recv).start()

    texts[0].wait()
    wait_for(kq, kq_recv)
    keyed = (((1,), (1,)), ((), ()))
    passes = [(t, lax.rem(chip + t, chips)) for t in list(range(1, chips)) + [0]]
    group = lax.div(s, per_chunk)
    for order, (t, owner) in enumerate(passes):
        blocks = [lax.rem(group + c + 1, chunks) * per_chunk for c in range(chunks)]
        for c, first in enumerate(blocks):
            q = kq[1, pl.ds(first, per_chunk), pl.ds(owner * CORES, CORES)]
            q = q.reshape(per_chunk * CORES * rows, HD)
            keys = kq[0].reshape(n_seq * n_head * rows, HD)
            on_video = lax.dot_general(q, keys, keyed, preferred_element_type=F32)
            on_text = lax.dot_general(q, tk[...], keyed, preferred_element_type=F32)
            top = jnp.maximum(
                jnp.max(on_video, axis=1, keepdims=True),
                jnp.max(on_text, axis=1, keepdims=True),
            )
            split = keys.shape[0]
            probs[c, :, :split] = jnp.exp2((on_video - top) * SCALE).astype(BF16)
            probs[c, :, split:] = jnp.exp2((on_text - top) * SCALE).astype(BF16)
        if order == 0:
            texts[1].wait()
            wait_for(vals, v_recv)
        for c, first in enumerate(blocks):
            values = vals[...].reshape(split, HD)
            ahead = jnp.dot(
                probs[c, :, :split],
                jnp.concatenate([values, jnp.ones_like(values)], axis=1),
                preferred_element_type=F32,
            ) + jnp.dot(
                probs[c, :, split:],
                jnp.concatenate([tv[...], jnp.ones_like(tv)], axis=1),
                preferred_element_type=F32,
            )
            done = (ahead[:, :HD] / ahead[:, HD:]).astype(BF16)
            att_send[t, c] = done.reshape(per_chunk, CORES * rows, HD)
            for b in range(per_chunk):
                here = lax.rem(s + b, per_chunk) if c == chunks - 1 else b
                src, dst = att_send.at[t, c, here], att.at[t, :, lanes(s)]
                if c == chunks - 1 and b == 0:
                    pltpu.make_async_copy(src, dst, att_rsem.at[t]).start()
                else:
                    send(src, dst, att_ssem.at[t], att_rsem.at[t], first + here, g)

    other = g + 1 - 2 * core
    crossing = []

    def project(t, n):
        if t == passes[0][0]:
            weights[n].wait()
        out = jnp.dot(att[t], w[:, cols(n)], preferred_element_type=F32).astype(BF16)
        part[t, :, :, cols(n)] = out.reshape(CORES, rows, width)
        return send(
            part.at[t, 1 - core, :, cols(n)], pair_in.at[t, :, cols(n)],
            pair_ssem.at[t, n], pair_rsem.at[t, n], s, other,
        )

    def own_sum(t, n, copy):
        copy.wait()
        return part[t, core, :, cols(n)].astype(F32) + pair_in[t, :, cols(n)].astype(F32)

    def cross(t, owner, n, copy):
        y_send[t - 1, :, cols(n)] = own_sum(t, n, copy).astype(BF16)
        crossing.append((t, n, send(
            y_send.at[t - 1, :, cols(n)], y_in.at[t - 1, :, cols(n)],
            y_ssem.at[t - 1, n], y_rsem.at[t - 1, n], s, owner * CORES + core,
        )))

    LAG = 2
    pending, last = [], []
    for t, owner in passes:
        wait_for(att.at[t], att_rsem.at[t])
        for n in range(n_cols):
            copy = project(t, n)
            if t == 0:
                last.append(copy)
            else:
                pending.append((t, owner, n, copy))
            if len(pending) > LAG or (t == 0 and pending):
                cross(*pending.pop(0))
    while pending:
        cross(*pending.pop(0))
    for n in range(n_cols):
        total = own_sum(0, n, last[n])
        for t, m, copy in crossing:
            if m == n:
                copy.wait()
                total = total + y_in[t - 1, :, cols(n)].astype(F32)
        o_ref[:, cols(n)] = total.astype(BF16)

    for i in range(2):
        wait_for(kq.at[i].reshape(n_seq * n_head, rows, HD).at[1:], kq_send)
    wait_for(vals.reshape(n_seq * n_head, rows, HD).at[1:], v_send)
    for t, owner in passes:
        wait_for(att.at[t, :, : (n_seq - 1) * HD], att_ssem.at[t])


def fused(n_seq, n_head, video_q, video_k, video_v, text_k, text_v, out_weight):
    rows, text = video_q.shape[0], text_k.shape[0]
    depth, d = out_weight.shape
    tokens = n_seq * n_head * rows
    chips = n_head // CORES
    per_chunk = 2
    chunks = n_seq // per_chunk
    m = per_chunk * CORES * rows
    n_cols = next(n for n in (5, 4, 8, 2, 1) if d % (n * 2 * HD) == 0)
    anywhere = pl.BlockSpec(memory_space=pl.ANY)
    dma = pltpu.SemaphoreType.DMA
    return pl.pallas_call(
        functools.partial(kernel, n_seq, n_head),
        out_shape=jax.ShapeDtypeStruct((rows, d), BF16),
        in_specs=[anywhere] * 6,
        out_specs=pl.BlockSpec(memory_space=pltpu.VMEM),
        scratch_shapes=[
            pltpu.VMEM((3, rows, video_q.shape[1]), BF16),
            pltpu.VMEM((2, n_seq, n_head, rows, HD), BF16),
            pltpu.VMEM((n_seq, n_head, rows, HD), BF16),
            pltpu.VMEM((text, HD), BF16),
            pltpu.VMEM((text, HD), BF16),
            pltpu.VMEM((depth, d), BF16),
            pltpu.VMEM((chunks, m, tokens + text), BF16),
            pltpu.VMEM((chips, chunks, per_chunk, CORES * rows, HD), BF16),
            pltpu.VMEM((chips, CORES * rows, depth), BF16),
            pltpu.VMEM((chips, CORES, rows, d), BF16),
            pltpu.VMEM((chips, rows, d), BF16),
            pltpu.VMEM((max(chips - 1, 1), rows, d), BF16),
            pltpu.VMEM((max(chips - 1, 1), rows, d), BF16),
            dma((3,)), dma((2,)), dma((n_cols,)),
            dma(()), dma(()), dma(()), dma(()),
            dma((chips,)), dma((chips,)),
            dma((chips, n_cols)), dma((chips, n_cols)),
            dma((chips, n_cols)), dma((chips, n_cols)),
        ],
        compiler_params=pltpu.CompilerParams(
            collective_id=0, has_side_effects=True, vmem_limit_bytes=60 * 2**20
        ),
    )(video_q, video_k, video_v, text_k, text_v, out_weight)


def as_heads(array):
    return array.reshape(array.shape[0], array.shape[1] // HD, HD)


def scores_of(query_heads, key_heads):
    return jnp.einsum(
        "qhd,khd->hqk", query_heads, key_heads, preferred_element_type=jnp.float32
    ) * HD ** (-0.5)


def weigh_values(scores, row_max, value_heads):
    weights = jnp.exp(scores - row_max[..., None]).astype(jnp.bfloat16)
    totals = jnp.sum(weights.astype(jnp.float32), axis=2)
    summed = jnp.einsum("hqk,khd->hqd", weights, value_heads, preferred_element_type=jnp.float32)
    return (totals, summed)


def local_partial(query_heads, key_heads, value_heads):
    scores = scores_of(query_heads, key_heads)
    row_max = jnp.max(scores, axis=2)
    totals, summed = weigh_values(scores, row_max, value_heads)
    return (row_max, totals, summed)


def combine_partial(first, second):
    joint = jnp.maximum(first[0], second[0])
    first_factor = jnp.exp(first[0] - joint)
    second_factor = jnp.exp(second[0] - joint)
    totals = first[1] * first_factor + second[1] * second_factor
    summed = first[2] * first_factor[..., None] + second[2] * second_factor[..., None]
    return (joint, totals, summed)


def body(video_q, video_k, video_v, text_k, text_v, out_weight):
    queries, key_rows, value_rows = (
        lax.all_to_all(video_q, "head", split_axis=1, concat_axis=0, tiled=True),
        lax.all_to_all(video_k, "head", split_axis=1, concat_axis=0, tiled=True),
        lax.all_to_all(video_v, "head", split_axis=1, concat_axis=0, tiled=True),
    )
    rows_here = queries.shape[0]
    query_heads = as_heads(queries)
    text_part = local_partial(query_heads, as_heads(text_k), as_heads(text_v))
    merged = combine_partial(
        text_part,
        local_partial(
            query_heads,
            as_heads(lax.all_gather(key_rows, "seq", axis=0, tiled=True)),
            as_heads(lax.all_gather(value_rows, "seq", axis=0, tiled=True)),
        ),
    )
    normalized = merged[2] / merged[1][..., None]
    attended = normalized.transpose(1, 0, 2).reshape(rows_here, -1).astype(jnp.bfloat16)
    return lax.psum_scatter(
        jnp.dot(attended, out_weight, preferred_element_type=jnp.float32).astype(jnp.bfloat16),
        "head",
        scatter_dimension=0,
        tiled=True,
    )


def solution(mesh):
    n_seq, n_head = mesh.shape["seq"], mesh.shape["head"]

    def step(*arrays):
        heads_here = arrays[3].shape[1] // HD
        one_head_each = heads_here == n_seq and n_seq % 2 == 0 and n_head % CORES == 0
        return fused(n_seq, n_head, *arrays) if one_head_each else body(*arrays)

    in_specs = (
        P(("seq", "head"), None),
        P(("seq", "head"), None),
        P(("seq", "head"), None),
        P(None, "head"),
        P(None, "head"),
        P("head", None),
    )
    out_specs = P(("seq", "head"), None)
    return jax.shard_map(step, mesh=mesh, in_specs=in_specs, out_specs=out_specs, check_vma=False)
```

```python
import functools
import math

import jax
import jax.numpy as jnp
from jax import lax
from jax.experimental import pallas as pl
from jax.experimental.pallas import tpu as pltpu
from jax.sharding import PartitionSpec as P

HD = 128
BF16 = jnp.bfloat16
F32 = jnp.float32
CORES = 2
SCALE = HD ** (-0.5) * math.log2(math.e)


def kernel(
    n_seq, n_head, q_ref, k_ref, v_ref, tk_ref, tv_ref, w_ref, o_ref,
    stage, keys_in, vals, queries, tk, tv, w, probs, att_send, att, part, pair_in, y_send, y_in,
    load_sem, text_sem, w_sem, k_send, k_recv, v_send, v_recv, q_send, q_recv,
    att_ssem, att_rsem, pair_ssem, pair_rsem, y_ssem, y_rsem,
):
    s, g = lax.axis_index("seq"), lax.axis_index("head")
    core, chip = lax.rem(g, CORES), lax.div(g, CORES)
    chips = n_head // CORES
    rows = q_ref.shape[0]
    n_cols = w_sem.shape[0]
    width = w_ref.shape[1] // n_cols
    per_chunk = probs.shape[1] // rows
    chunks = n_seq // per_chunk
    split = n_seq * n_head * rows

    def lanes(block):
        return pl.ds(pl.multiple_of(block * HD, HD), HD)

    def cols(n):
        return pl.ds(n * width, width)

    loads = [
        pltpu.make_async_copy(ref, stage.at[i], load_sem.at[i])
        for i, ref in enumerate((k_ref, q_ref, v_ref))
    ]
    texts = [
        pltpu.make_async_copy(tk_ref.at[:, lanes(s)], tk, text_sem.at[0]),
        pltpu.make_async_copy(tv_ref.at[:, lanes(s)], tv, text_sem.at[1]),
    ]
    weights = [
        pltpu.make_async_copy(w_ref.at[:, cols(n)], w.at[:, cols(n)], w_sem.at[n])
        for n in range(n_cols)
    ]
    for copy in loads + texts + weights:
        copy.start()

    turns = list(range(1, chips)) + [0]
    offsets = list(range(n_seq))

    def targets(turn):
        return [
            (lax.rem(s + o, n_seq), lax.rem(chip + chips - turn, chips) * CORES + lax.rem(core + c, CORES))
            for o in offsets for c in range(CORES) if (turn, o, c) != (0, 0, 0)
        ]

    others = [
        (lax.rem(s + o, n_seq), lax.rem(chip + chips - turn, chips) * CORES + lax.rem(core + c, CORES))
        for o in offsets for turn in turns for c in range(CORES) if (turn, o, c) != (0, 0, 0)
    ]
    barrier = pltpu.get_barrier_semaphore()
    for ts, tg in others:
        pl.semaphore_signal(
            barrier, inc=1, device_id={"seq": ts, "head": tg},
            device_id_type=pl.DeviceIdType.MESH,
        )
    pl.semaphore_wait(barrier, len(others))

    def send(src, dst, ssem, rsem, ts, tg):
        return pltpu.make_async_remote_copy(
            src_ref=src, dst_ref=dst, send_sem=ssem, recv_sem=rsem,
            device_id={"seq": ts, "head": tg}, device_id_type=pl.DeviceIdType.MESH,
        )

    def wait_for(ref, sem):
        pltpu.make_async_copy(ref, ref, sem).wait()

    mine = lanes(g * n_seq + s)

    def spread(i, buffer, ssem, rsem, to):
        for ts, tg in to:
            send(stage.at[i, :, lanes(tg * n_seq + ts)], buffer.at[s, g], ssem, rsem, ts, tg).start()

    loads[0].wait()
    spread(0, keys_in, k_send, k_recv, others)
    pltpu.make_async_copy(stage.at[0, :, mine], keys_in.at[s, g], k_recv).start()
    loads[1].wait()
    for turn in turns[:-1]:
        spread(1, queries, q_send.at[turn], q_recv.at[turn], targets(turn))
    loads[2].wait()
    spread(2, vals, v_send, v_recv, others)
    pltpu.make_async_copy(stage.at[2, :, mine], vals.at[s, g], v_recv).start()
    spread(1, queries, q_send.at[0], q_recv.at[0], targets(0))
    pltpu.make_async_copy(stage.at[1, :, mine], queries.at[s, g], q_recv.at[0]).start()

    texts[0].wait()
    wait_for(keys_in, k_recv)
    keyed = (((1,), (1,)), ((), ()))
    group = lax.div(s, per_chunk)
    blocks = [lax.rem(group + c + 1, chunks) * per_chunk for c in range(chunks)]
    owners = [(t, lax.rem(chip + t, chips)) for t in turns]
    passes = [(t, owner, cc) for t, owner in owners for cc in range(CORES)]
    for order, (t, owner, cc) in enumerate(passes):
        if cc == 0:
            wait_for(queries.at[:, pl.ds(owner * CORES, CORES)], q_recv.at[t])
        for c, first in enumerate(blocks):
            q = queries[pl.ds(first, per_chunk), owner * CORES + cc].reshape(per_chunk * rows, HD)
            keys = keys_in[...].reshape(split, HD)
            on_video = lax.dot_general(q, keys, keyed, preferred_element_type=F32)
            on_text = lax.dot_general(q, tk[...], keyed, preferred_element_type=F32)
            top = jnp.maximum(
                jnp.max(on_video, axis=1, keepdims=True),
                jnp.max(on_text, axis=1, keepdims=True),
            )
            probs[c, :, :split] = jnp.exp2((on_video - top) * SCALE).astype(BF16)
            probs[c, :, split:] = jnp.exp2((on_text - top) * SCALE).astype(BF16)
        if order == 0:
            texts[1].wait()
            wait_for(vals, v_recv)
        for c, first in enumerate(blocks):
            values = vals[...].reshape(split, HD)
            ahead = jnp.dot(
                probs[c, :, :split],
                jnp.concatenate([values, jnp.ones_like(values)], axis=1),
                preferred_element_type=F32,
            ) + jnp.dot(
                probs[c, :, split:],
                jnp.concatenate([tv[...], jnp.ones_like(tv)], axis=1),
                preferred_element_type=F32,
            )
            done = (ahead[:, :HD] / ahead[:, HD:]).astype(BF16)
            att_send[t, cc, c] = done.reshape(per_chunk, rows, HD)
            for b in range(per_chunk):
                here = lax.rem(s + b, per_chunk) if c == chunks - 1 else b
                src, dst = att_send.at[t, cc, c, here], att.at[t, cc, :, lanes(s)]
                if c == chunks - 1 and b == 0:
                    pltpu.make_async_copy(src, dst, att_rsem.at[t, cc]).start()
                else:
                    send(src, dst, att_ssem.at[t, cc], att_rsem.at[t, cc], first + here, g).start()

    def to_pair(t, n):
        return send(
            part.at[t, 1 - core, :, cols(n)], pair_in.at[t, :, cols(n)],
            pair_ssem.at[t, n], pair_rsem.at[t, n], s, g + 1 - 2 * core,
        )

    def to_owner(t, owner, n):
        return send(
            y_send.at[t - 1, :, cols(n)], y_in.at[t - 1, :, cols(n)],
            y_ssem.at[t - 1, n], y_rsem.at[t - 1, n], s, owner * CORES + core,
        )

    def own_sum(t, n):
        to_pair(t, n).wait_recv()
        return part[t, core, :, cols(n)].astype(F32) + pair_in[t, :, cols(n)].astype(F32)

    def cross(t, owner, cc, n):
        @pl.when(core == cc)
        def _():
            y_send[t - 1, :, cols(n)] = own_sum(t, n).astype(BF16)
            to_owner(t, owner, n).start()

    LAG = 2
    pending = []
    for order, (t, owner, cc) in enumerate(passes):
        wait_for(att.at[t, cc], att_rsem.at[t, cc])
        for n in range(n_cols):
            if order == 0:
                weights[n].wait()
            part[t, cc, :, cols(n)] = jnp.dot(
                att[t, cc], w[:, cols(n)], preferred_element_type=F32
            ).astype(BF16)

            @pl.when(core != cc)
            def _():
                to_pair(t, n).start()

            if t > 0:
                pending.append((t, owner, cc, n))
            if pending and (len(pending) > LAG or t == 0):
                cross(*pending.pop(0))
    while pending:
        cross(*pending.pop(0))
    for n in range(n_cols):
        total = own_sum(0, n)
        for t, owner in owners[:-1]:
            to_owner(t, owner, n).wait_recv()
            total = total + y_in[t - 1, :, cols(n)].astype(F32)
        o_ref[:, cols(n)] = total.astype(BF16)

    for buffer, sem in ((keys_in, k_send), (vals, v_send)):
        wait_for(buffer.reshape(n_seq * n_head, rows, HD).at[1:], sem)
    for t, owner in owners:
        sent = n_seq * CORES - (t == 0)
        wait_for(queries.reshape(n_seq * n_head, rows, HD).at[:sent], q_send.at[t])
        for cc in range(CORES):
            wait_for(att.at[t, cc, :, : (n_seq - 1) * HD], att_ssem.at[t, cc])
        for n in range(n_cols):
            to_pair(t, n).wait_send()
            if t > 0:
                to_owner(t, owner, n).wait_send()


def fused(n_seq, n_head, video_q, video_k, video_v, text_k, text_v, out_weight):
    rows, text = video_q.shape[0], text_k.shape[0]
    depth, d = out_weight.shape
    tokens = n_seq * n_head * rows
    chips = n_head // CORES
    per_chunk = next(c for c in (4, 2, 1) if n_seq % c == 0)
    chunks = n_seq // per_chunk
    m = per_chunk * rows
    n_cols = next(n for n in (4, 5, 8, 2, 1) if d % (n * 2 * HD) == 0)
    anywhere = pl.BlockSpec(memory_space=pl.ANY)
    dma = pltpu.SemaphoreType.DMA
    return pl.pallas_call(
        functools.partial(kernel, n_seq, n_head),
        out_shape=jax.ShapeDtypeStruct((rows, d), BF16),
        in_specs=[anywhere] * 6,
        out_specs=pl.BlockSpec(memory_space=pltpu.VMEM),
        scratch_shapes=[
            pltpu.VMEM((3, rows, video_q.shape[1]), BF16),
            pltpu.VMEM((n_seq, n_head, rows, HD), BF16),
            pltpu.VMEM((n_seq, n_head, rows, HD), BF16),
            pltpu.VMEM((n_seq, n_head, rows, HD), BF16),
            pltpu.VMEM((text, HD), BF16),
            pltpu.VMEM((text, HD), BF16),
            pltpu.VMEM((depth, d), BF16),
            pltpu.VMEM((chunks, m, tokens + text), BF16),
            pltpu.VMEM((chips, CORES, chunks, per_chunk, rows, HD), BF16),
            pltpu.VMEM((chips, CORES, rows, depth), BF16),
            pltpu.VMEM((chips, CORES, rows, d), BF16),
            pltpu.VMEM((chips, rows, d), BF16),
            pltpu.VMEM((max(chips - 1, 1), rows, d), BF16),
            pltpu.VMEM((max(chips - 1, 1), rows, d), BF16),
            dma((3,)), dma((2,)), dma((n_cols,)),
            dma(()), dma(()), dma(()), dma(()), dma((chips,)), dma((chips,)),
            dma((chips, CORES)), dma((chips, CORES)),
            dma((chips, n_cols)), dma((chips, n_cols)),
            dma((chips, n_cols)), dma((chips, n_cols)),
        ],
        compiler_params=pltpu.CompilerParams(
            collective_id=0, has_side_effects=True, vmem_limit_bytes=60 * 2**20
        ),
    )(video_q, video_k, video_v, text_k, text_v, out_weight)


def as_heads(array):
    return array.reshape(array.shape[0], array.shape[1] // HD, HD)


def scores_of(query_heads, key_heads):
    return jnp.einsum(
        "qhd,khd->hqk", query_heads, key_heads, preferred_element_type=jnp.float32
    ) * HD ** (-0.5)


def weigh_values(scores, row_max, value_heads):
    weights = jnp.exp(scores - row_max[..., None]).astype(jnp.bfloat16)
    totals = jnp.sum(weights.astype(jnp.float32), axis=2)
    summed = jnp.einsum("hqk,khd->hqd", weights, value_heads, preferred_element_type=jnp.float32)
    return (totals, summed)


def local_partial(query_heads, key_heads, value_heads):
    scores = scores_of(query_heads, key_heads)
    row_max = jnp.max(scores, axis=2)
    totals, summed = weigh_values(scores, row_max, value_heads)
    return (row_max, totals, summed)


def combine_partial(first, second):
    joint = jnp.maximum(first[0], second[0])
    first_factor = jnp.exp(first[0] - joint)
    second_factor = jnp.exp(second[0] - joint)
    totals = first[1] * first_factor + second[1] * second_factor
    summed = first[2] * first_factor[..., None] + second[2] * second_factor[..., None]
    return (joint, totals, summed)


def body(video_q, video_k, video_v, text_k, text_v, out_weight):
    queries, key_rows, value_rows = (
        lax.all_to_all(video_q, "head", split_axis=1, concat_axis=0, tiled=True),
        lax.all_to_all(video_k, "head", split_axis=1, concat_axis=0, tiled=True),
        lax.all_to_all(video_v, "head", split_axis=1, concat_axis=0, tiled=True),
    )
    rows_here = queries.shape[0]
    query_heads = as_heads(queries)
    text_part = local_partial(query_heads, as_heads(text_k), as_heads(text_v))
    merged = combine_partial(
        text_part,
        local_partial(
            query_heads,
            as_heads(lax.all_gather(key_rows, "seq", axis=0, tiled=True)),
            as_heads(lax.all_gather(value_rows, "seq", axis=0, tiled=True)),
        ),
    )
    normalized = merged[2] / merged[1][..., None]
    attended = normalized.transpose(1, 0, 2).reshape(rows_here, -1).astype(jnp.bfloat16)
    return lax.psum_scatter(
        jnp.dot(attended, out_weight, preferred_element_type=jnp.float32).astype(jnp.bfloat16),
        "head",
        scatter_dimension=0,
        tiled=True,
    )


def solution(mesh):
    n_seq, n_head = mesh.shape["seq"], mesh.shape["head"]

    def step(*arrays):
        heads_here = arrays[3].shape[1] // HD
        one_head_each = heads_here == n_seq and n_head % CORES == 0
        return fused(n_seq, n_head, *arrays) if one_head_each else body(*arrays)

    in_specs = (
        P(("seq", "head"), None),
        P(("seq", "head"), None),
        P(("seq", "head"), None),
        P(None, "head"),
        P(None, "head"),
        P("head", None),
    )
    out_specs = P(("seq", "head"), None)
    return jax.shard_map(step, mesh=mesh, in_specs=in_specs, out_specs=out_specs, check_vma=False)
```
